32 devices in a mesh: dp: 2 (over x), ep: 16 (over y, z, core).
Axes of the slice: x: 2, y: 2, z: 4, core: 2. Of those that a mesh axis runs over, the one named last changes fastest.
Arguments:
- x: bfloat16 [2, 16, 256, 1536], P('dp', 'ep'), parts along dimension 0
- expert: int32 [2, 16, 256, 2], P('dp', 'ep'), parts along dimension 0
- slot: int32 [2, 16, 256, 2], P('dp', 'ep'), parts along dimension 0
- gate: float32 [2, 16, 256, 2], P('dp', 'ep'), parts along dimension 0
- w_gate: bfloat16 [32, 1536, 9216], P('ep')
- w_up: bfloat16 [32, 1536, 9216], P('ep')
- w_down: bfloat16 [32, 9216, 1536], P('ep')
Outputs:
- y: bfloat16 [2, 16, 256, 1536], P('dp', 'ep'), parts along dimension 0
There are 2 independent parts. The reference program is written for one: setup_inputs(seed, part) draws one part's arguments, and reference() takes and returns one part's arrays. A program takes and returns all parts, laid end to end along the dimension named above; an argument that names none is the same for every part.
All inputs are finite; a program needn't handle non-finite values.
Results may differ from the reference program's by a relative error of at most 0.009.
Values are sent between devices in bfloat16 or wider.
A program may use at most 2 GiB of HBM per device.

```python
import jax
import jax.numpy as jnp

MEMBERS = 16
TOKENS = 256
D = 1536
FF = 9216
TOP = 2
EXPERTS = 32
SLOTS = 5 * TOKENS * TOP // (4 * EXPERTS)


def setup_inputs(seed: int = 0, part: int = 0) -> dict:
    own, k1, k2, k3, k4, k5, k6 = jax.random.split(jax.random.key(seed), 7)
    kx, ke, kl, kg = jax.random.split(jax.random.fold_in(own, part), 4)
    devices = (1, MEMBERS)
    place = jax.random.permutation(kl, jnp.arange(EXPERTS, dtype=jnp.uint32))
    slow = ((EXPERTS + (9 * place) % EXPERTS) << ((9 * place) // EXPERTS)) // EXPERTS
    wait = (jax.random.bits(ke, (*devices, TOKENS, EXPERTS), jnp.uint32) >> 10) * slow
    expert = jnp.argsort(wait, axis=-1)[..., :TOP].astype(jnp.int32)
    chosen = jax.nn.one_hot(expert, EXPERTS, dtype=jnp.int32)
    in_line = jnp.cumsum(chosen.reshape(*devices, TOKENS * TOP, EXPERTS), axis=2) - 1
    slot = jnp.sum(in_line.reshape(chosen.shape) * chosen, axis=-1)

    def one(key, rows, columns):
        return (jax.random.normal(key, (rows, columns), jnp.float32) * rows**-0.5).astype(jnp.bfloat16)

    def weights(key, rows, columns):
        return jax.lax.map(lambda k: one(k, rows, columns), jax.random.split(key, EXPERTS))

    return {
        "x": jax.random.normal(kx, (*devices, TOKENS, D), jnp.float32).astype(jnp.bfloat16),
        "expert": expert,
        "slot": slot,
        "gate": jax.nn.softmax(jax.random.normal(kg, expert.shape, jnp.float32)),
        "w_gate": weights(k1, D, FF),
        "w_up": weights(k2, D, FF),
        "w_down": weights(k3, FF, D),
    }


def einsum(form, a, b):
    return jnp.einsum(form, a.astype(jnp.float32), b.astype(jnp.float32))


def reference(x, expert, slot, gate, w_gate, w_up, w_down):
    to_expert = jax.nn.one_hot(expert, EXPERTS, dtype=jnp.bfloat16)
    to_slot = jax.nn.one_hot(slot, SLOTS, dtype=jnp.bfloat16)
    weighted = to_expert * gate[..., None].astype(jnp.bfloat16)
    dispatch = einsum("abtke,abtkc->abtec", to_expert, to_slot).astype(jnp.bfloat16)
    combine = einsum("abtke,abtkc->abtec", weighted, to_slot).astype(jnp.bfloat16)
    z = einsum("abtec,abtd->aebcd", dispatch, x).astype(jnp.bfloat16)
    h = jax.nn.silu(einsum("aebcd,edf->aebcf", z, w_gate))
    h = (h * einsum("aebcd,edf->aebcf", z, w_up)).astype(jnp.bfloat16)
    out = einsum("aebcf,efd->aebcd", h, w_down).astype(jnp.bfloat16)
    y = einsum("abtec,aebcd->abtd", combine, out)
    return y.astype(jnp.bfloat16)
```

```python
import functools

import jax
import jax.numpy as jnp
from jax import lax
from jax.experimental import pallas as pl
from jax.experimental.pallas import tpu as pltpu
from jax.sharding import PartitionSpec as P

MESH = pl.DeviceIdType.MESH
N = 16
C = 20
T, D, F = 256, 1536, 9216
HD = D // 2
QD = HD // 2
NBUF = 4
TF = 1024
NJ = F // TF
OC = 512
NC = D // OC
NK = 3
PER = 2 * NJ + NC * NK
STEPS = 2 * PER
ROWS = N * C


def swap(a, b, first):
    return jnp.where(first, a, pltpu.roll(b, C, 0)), jnp.where(first, pltpu.roll(a, C, 0), b)


def peer(me, k):
    y, z, c = me // 8, (me // 2) % 4, me % 2
    half = (z // 2 + (k // 8) + 1) % 2
    zz = half * 2 + (z + k // 2) % 2
    return ((y + (k // 4)) % 2) * 8 + zz * 2 + (c + k) % 2


def kernel(
    expert_ref, slot_ref, gate_ref, x_ref, wg, wu, wd, y_ref,
    send, recv, rsend, rrecv, zbuf, zl, acc, h, oacc, obuf, ct, wbuf,
    wsem, ssem, rsem, rssem, rrsem,
):
    dp, me = lax.axis_index("dp"), lax.axis_index("ep")

    def fetch(n):
        s = n % NBUF
        e, r = n // PER, n % PER

        @pl.when(r < 2 * NJ)
        def _():
            hf, j = r // NJ, r % NJ
            rows = pl.ds(hf * HD, HD)
            for q in range(4):
                w = wg if q < 2 else wu
                cols = pl.ds(j * TF + (q % 2) * 512, 512)
                pltpu.make_async_copy(w.at[e, rows, cols], wbuf.at[s, q], wsem.at[s, q]).start()

        @pl.when(r >= 2 * NJ)
        def _():
            c, k = (r - 2 * NJ) // NK, (r - 2 * NJ) % NK
            for q in range(4):
                rows = pl.ds(k * 4 * HD + q * HD, HD)
                cols = pl.ds(c * OC, OC)
                pltpu.make_async_copy(wd.at[e, rows, cols], wbuf.at[s, q], wsem.at[s, q]).start()

    def arrived(n):
        s = n % NBUF
        for q in range(4):
            pltpu.make_async_copy(wg.at[0, pl.ds(0, HD), pl.ds(0, 512)], wbuf.at[s, q], wsem.at[s, q]).wait()
        return s

    def refill(n):
        @pl.when(n + NBUF < STEPS)
        def _():
            fetch(n + NBUF)

    barrier = pltpu.get_barrier_semaphore()

    @pl.loop(1, N)
    def _(k):
        pl.semaphore_signal(barrier, inc=1, device_id=(dp, (me + k) % N), device_id_type=MESH)

    @pl.loop(0, NBUF)
    def _(n):
        fetch(n)

    key = jnp.where(slot_ref[...] < C, expert_ref[...] * C + slot_ref[...], -1)
    k0, k1 = key[0:1, :], key[1:2, :]
    gate = gate_ref[...].astype(jnp.bfloat16).astype(jnp.float32)
    row = lax.broadcasted_iota(jnp.int32, (2 * ROWS, T), 0)
    hit0, hit1 = k0 == row, k1 == row
    pick = (jnp.where(hit0, 1.0, 0.0) + jnp.where(hit1, 1.0, 0.0)).astype(jnp.bfloat16)
    weighted = jnp.where(hit0, gate[0:1, :], 0.0) + jnp.where(hit1, gate[1:2, :], 0.0)
    ct[...] = weighted.astype(jnp.bfloat16)
    first_q = lax.broadcasted_iota(jnp.int32, (2 * C, QD), 0) < C
    first_o = lax.broadcasted_iota(jnp.int32, (2 * C, OC // 2), 0) < C

    def dispatch(e, hf, k):
        to = peer(me, k)
        return pltpu.make_async_remote_copy(
            send.at[e, hf, to], recv.at[e, hf, me], ssem.at[e, hf, to], rsem.at[e, hf, me],
            device_id=(dp, to), device_id_type=MESH,
        )

    def send_all(e, hf):
        @pl.loop(0, N - 1)
        def _(i):
            dispatch(e, hf, i + i // 8).start()

        recv[e, hf, me] = send[e, hf, me]

    for hf in range(2):
        zbuf[...] = jnp.dot(pick, x_ref[:, hf * HD : (hf + 1) * HD], preferred_element_type=jnp.float32)

        @pl.loop(0, N)
        def _(d):
            rows = pl.ds(pl.multiple_of(d * 2 * C, 8), 2 * C)
            a, b = swap(zbuf[rows, :QD], zbuf[rows, QD:], first_q)
            send[0, hf, d] = a.astype(jnp.bfloat16)
            send[1, hf, d] = b.astype(jnp.bfloat16)

        if hf == 0:
            pl.semaphore_wait(barrier, N - 1)
        send_all(0, hf)
    send_all(1, 0)
    send_all(1, 1)

    def gathered(e, hf):
        @pl.loop(0, N - 1)
        def _(i):
            src = (me + 1 + i) % N
            pltpu.make_async_remote_copy(
                send.at[e, hf, src], recv.at[e, hf, src], ssem.at[e, hf, src], rsem.at[e, hf, src],
                device_id=(dp, src), device_id_type=MESH,
            ).wait_recv()

        @pl.loop(0, N // 4)
        def _(p):
            blocks = [recv[e, hf, 4 * p + i].astype(jnp.float32) for i in range(4)]
            l0, h0 = swap(blocks[0], blocks[1], first_q)
            l1, h1 = swap(blocks[2], blocks[3], first_q)
            rows = pl.ds(pl.multiple_of(p * 4 * C, 16), 4 * C)
            zl[rows, :QD] = jnp.concatenate([l0, l1], axis=0).astype(jnp.bfloat16)
            zl[rows, QD:] = jnp.concatenate([h0, h1], axis=0).astype(jnp.bfloat16)

    def back(e, c, k):
        to = peer(me, k)
        return pltpu.make_async_remote_copy(
            rsend.at[e, c, to], rrecv.at[e, c, me], rssem.at[e, c, to], rrsem.at[e, c, me],
            device_id=(dp, to), device_id_type=MESH,
        )

    dot = functools.partial(jnp.dot, preferred_element_type=jnp.float32)

    @pl.loop(0, 2)
    def _(e):
        gathered(e, 0)

        @pl.loop(0, NJ)
        def _(j):
            n = e * PER + j
            s = arrived(n)
            for q in range(4):
                acc[j, q] = dot(zl[...], wbuf[s, q])
            refill(n)

        gathered(e, 1)

        @pl.loop(0, NJ)
        def _(j):
            n = e * PER + NJ + j
            s = arrived(n)
            for q in range(2):
                g = acc[j, q] + dot(zl[...], wbuf[s, q])
                u = acc[j, q + 2] + dot(zl[...], wbuf[s, q + 2])
                h[j, q] = (g * jax.nn.sigmoid(g) * u).astype(jnp.bfloat16)
            refill(n)

        @pl.loop(0, NC)
        def _(c):
            @pl.loop(0, NK)
            def _(k):
                n = e * PER + 2 * NJ + c * NK + k
                s = arrived(n)
                total = jnp.zeros((ROWS, OC), jnp.float32)
                for q in range(4):
                    at = [q * HD + o for o in range(0, HD, 256)]
                    left = [h[3 * k + o // TF, o % TF // 512, :, o % 512 : o % 512 + 256] for o in at]
                    total += dot(jnp.concatenate(left, axis=1), wbuf[s, q])

                @pl.when(k == 0)
                def _():
                    oacc[...] = total

                @pl.when(k > 0)
                def _():
                    oacc[...] += total

                refill(n)

            @pl.loop(0, N // 2)
            def _(p):
                rows = pl.ds(pl.multiple_of(p * 2 * C, 8), 2 * C)
                a, b = swap(oacc[rows, : OC // 2], oacc[rows, OC // 2 :], first_o)
                rsend[e, c, 2 * p] = a.astype(jnp.bfloat16)
                rsend[e, c, 2 * p + 1] = b.astype(jnp.bfloat16)

            @pl.loop(0, N - 1)
            def _(i):
                back(e, c, i + i // 8).start()

            rrecv[e, c, me] = rsend[e, c, me]

    for c in range(NC):
        @pl.loop(0, N - 1)
        def _(i):
            src = (me + 1 + i) % N
            for e in range(2):
                pltpu.make_async_remote_copy(
                    rsend.at[e, c, src], rrecv.at[e, c, src], rssem.at[e, c, src], rrsem.at[e, c, src],
                    device_id=(dp, src), device_id_type=MESH,
                ).wait_recv()

        @pl.loop(0, N // 2)
        def _(p):
            parts = [
                swap(rrecv[0, c, 2 * p + i].astype(jnp.float32), rrecv[1, c, 2 * p + i].astype(jnp.float32), first_o)
                for i in range(2)
            ]
            rows = pl.ds(pl.multiple_of(p * 4 * C, 16), 4 * C)
            for i in range(2):
                obuf[rows, i * (OC // 2) : (i + 1) * (OC // 2)] = jnp.concatenate(
                    [parts[0][i], parts[1][i]], axis=0
                ).astype(jnp.bfloat16)

        y_ref[:, c * OC : (c + 1) * OC] = lax.dot_general(
            ct[...], obuf[...], (((0,), (0,)), ((), ())), preferred_element_type=jnp.float32
        ).astype(jnp.bfloat16)

    @pl.loop(0, N - 1)
    def _(i):
        k = i + i // 8
        for e in range(2):
            for hf in range(2):
                dispatch(e, hf, k).wait_send()
            for c in range(NC):
                back(e, c, k).wait_send()


def solution(mesh):
    spec = P("dp", "ep")

    def layer(x, expert, slot, gate, w_gate, w_up, w_down):
        vmem = pl.BlockSpec(memory_space=pltpu.VMEM)
        hbm = pl.BlockSpec(memory_space=pl.ANY)
        bf16, f32 = jnp.bfloat16, jnp.float32
        dma = pltpu.SemaphoreType.DMA
        y = pl.pallas_call(
            kernel,
            out_shape=jax.ShapeDtypeStruct((T, D), bf16),
            in_specs=[vmem] * 4 + [hbm] * 3,
            out_specs=vmem,
            scratch_shapes=[
                pltpu.VMEM((2, 2, N, 2 * C, QD), bf16),
                pltpu.VMEM((2, 2, N, 2 * C, QD), bf16),
                pltpu.VMEM((2, NC, N, 2 * C, OC // 2), bf16),
                pltpu.VMEM((2, NC, N, 2 * C, OC // 2), bf16),
                pltpu.VMEM((2 * ROWS, HD), f32),
                pltpu.VMEM((ROWS, HD), bf16),
                pltpu.VMEM((NJ, 4, ROWS, 512), f32),
                pltpu.VMEM((NJ, 2, ROWS, 512), bf16),
                pltpu.VMEM((ROWS, OC), f32),
                pltpu.VMEM((2 * ROWS, OC), bf16),
                pltpu.VMEM((2 * ROWS, T), bf16),
                pltpu.VMEM((NBUF, 4, HD, 512), bf16),
                dma((NBUF, 4)),
                dma((2, 2, N)),
                dma((2, 2, N)),
                dma((2, NC, N)),
                dma((2, NC, N)),
            ],
            compiler_params=pltpu.CompilerParams(
                collective_id=0, has_side_effects=True, vmem_limit_bytes=66_000_000
            ),
            name="moe",
        )(
            expert.reshape(T, 2).T, slot.reshape(T, 2).T, gate.reshape(T, 2).T,
            x.reshape(T, D), w_gate, w_up, w_down,
        )
        return y.reshape(1, 1, T, D)

    return jax.shard_map(
        layer, mesh=mesh,
        in_specs=(spec, spec, spec, spec, P("ep"), P("ep"), P("ep")),
        out_specs=spec, check_vma=False,
    )
```

```python
import functools

import jax
import jax.numpy as jnp
from jax import lax
from jax.experimental import pallas as pl
from jax.experimental.pallas import tpu as pltpu
from jax.sharding import PartitionSpec as P

MESH = pl.DeviceIdType.MESH
N = 16
C = 20
T, D, F = 256, 1536, 9216
NH = 3
KD = D // NH
QD = KD // 2
TF = 512
NJ = F // TF
NK = 9
GU, GW = 9, 9
NBUF = NJ
PER = NH * (NJ + NK)
ROWS = N * C


def swap(a, b, first):
    return jnp.where(first, a, pltpu.roll(b, C, 0)), jnp.where(first, pltpu.roll(a, C, 0), b)


def peer(me, k):
    y, z, c = me // 8, (me // 2) % 4, me % 2
    half = (z // 2 + (k // 8) + 1) % 2
    zz = half * 2 + (z + k // 2) % 2
    return ((y + (k // 4)) % 2) * 8 + zz * 2 + (c + k) % 2


def kernel(
    expert_ref, slot_ref, gate_ref, x_ref, wg, wu, wd, y_ref,
    send, recv, rsend, rrecv, zbuf, zl, acc, h, oacc, obuf, ct, wbuf,
    wsem, ssem, rsem, rssem, rrsem,
):
    dp, me = lax.axis_index("dp"), lax.axis_index("ep")
    dot = functools.partial(jnp.dot, preferred_element_type=jnp.float32)

    def fetch_up(e, part, j, s):
        rows, cols = pl.ds(part * KD, KD), pl.ds(j * TF, TF)
        pltpu.make_async_copy(wg.at[e, rows, cols], wbuf.at[s, 0], wsem.at[s, 0]).start()
        pltpu.make_async_copy(wu.at[e, rows, cols], wbuf.at[s, 1], wsem.at[s, 1]).start()

    def fetch_down(e, c, k, s):
        for q in range(2):
            rows, cols = pl.ds((k * 2 + q) * TF, TF), pl.ds(c * KD, KD)
            pltpu.make_async_copy(wd.at[e, rows, cols], wbuf.at[s, q], wsem.at[s, q]).start()

    def arrived(slots):
        for s in slots:
            for q in range(2):
                pltpu.make_async_copy(
                    wg.at[0, pl.ds(0, KD), pl.ds(0, TF)], wbuf.at[s, q], wsem.at[s, q]
                ).wait()

    barrier = pltpu.get_barrier_semaphore()

    @pl.loop(1, N)
    def _(k):
        pl.semaphore_signal(barrier, inc=1, device_id=(dp, (me + k) % N), device_id_type=MESH)

    @pl.loop(0, NBUF)
    def _(n):
        fetch_up(0, 0, n, n)

    key = jnp.where(slot_ref[...] < C, expert_ref[...] * C + slot_ref[...], -1)
    k0, k1 = key[0:1, :], key[1:2, :]
    gate = gate_ref[...].astype(jnp.bfloat16).astype(jnp.float32)
    row = lax.broadcasted_iota(jnp.int32, (2 * ROWS, T), 0)
    hit0, hit1 = k0 == row, k1 == row
    pick = (jnp.where(hit0, 1.0, 0.0) + jnp.where(hit1, 1.0, 0.0)).astype(jnp.bfloat16)
    weighted = jnp.where(hit0, gate[0:1, :], 0.0) + jnp.where(hit1, gate[1:2, :], 0.0)
    ct[...] = weighted.astype(jnp.bfloat16)
    first = lax.broadcasted_iota(jnp.int32, (2 * C, QD), 0) < C

    def dispatch(e, part, k):
        to = peer(me, k)
        return pltpu.make_async_remote_copy(
            send.at[e, part, to], recv.at[e, part, me], ssem.at[e, part, to], rsem.at[e, part, me],
            device_id=(dp, to), device_id_type=MESH,
        )

    def send_all(e, part):
        for i in range(N - 1):
            dispatch(e, part, i + i // 8).start()

    def receive(e, part):
        @pl.loop(0, N - 1)
        def _(i):
            src = (me + 1 + i) % N
            pltpu.make_async_remote_copy(
                send.at[e, part, src], recv.at[e, part, src], ssem.at[e, part, src], rsem.at[e, part, src],
                device_id=(dp, src), device_id_type=MESH,
            ).wait_recv()

    for part in range(NH):
        zbuf[...] = dot(pick, x_ref[:, part * KD : (part + 1) * KD])

        @pl.loop(0, N)
        def _(d):
            rows = pl.ds(pl.multiple_of(d * 2 * C, 8), 2 * C)
            a, b = swap(zbuf[rows, :QD], zbuf[rows, QD:], first)
            send[0, part, d] = a.astype(jnp.bfloat16)
            send[1, part, d] = b.astype(jnp.bfloat16)

        for e in range(2):
            recv[e, part, me] = send[e, part, me]

    pl.semaphore_wait(barrier, N - 1)
    for part in range(NH):
        send_all(0, part)

    def gathered(e, part):
        receive(e, part)

        if part == 1:

            @pl.when(e == 0)
            def _():
                for later in range(NH):
                    send_all(1, later)

        @pl.loop(0, N // 4)
        def _(p):
            blocks = [recv[e, part, 4 * p + i].astype(jnp.float32) for i in range(4)]
            l0, h0 = swap(blocks[0], blocks[1], first)
            l1, h1 = swap(blocks[2], blocks[3], first)
            rows = pl.ds(pl.multiple_of(p * 4 * C, 16), 4 * C)
            zl[rows, :QD] = jnp.concatenate([l0, l1], axis=0).astype(jnp.bfloat16)
            zl[rows, QD:] = jnp.concatenate([h0, h1], axis=0).astype(jnp.bfloat16)

    def back(e, c, k):
        to = peer(me, k)
        return pltpu.make_async_remote_copy(
            rsend.at[e, c, to], rrecv.at[e, c, me], rssem.at[e, c, to], rrsem.at[e, c, me],
            device_id=(dp, to), device_id_type=MESH,
        )

    @pl.loop(0, 2)
    def _(e):
        for part in range(NH):
            gathered(e, part)

            @pl.loop(0, NJ // GU)
            def _(t):
                n = e * PER + part * NJ + t * GU
                for w in range(0, GU, GW):
                    slots = [(n + w + i) % NBUF for i in range(GW)]
                    arrived(slots)
                    for i, s in enumerate(slots):
                        j = t * GU + w + i
                        g, u = dot(zl[...], wbuf[s, 0]), dot(zl[...], wbuf[s, 1])
                        if part > 0:
                            g, u = acc[j, 0] + g, acc[j, 1] + u
                        if part < NH - 1:
                            acc[j, 0], acc[j, 1] = g, u
                            fetch_up(e, part + 1, j, s)
                        else:
                            h[j] = (g * jax.nn.sigmoid(g) * u).astype(jnp.bfloat16)
                            fetch_down(e, j // NK, j % NK, s)

        for c in range(NH):
            n = e * PER + NH * NJ + c * NK
            total = None
            for w in range(0, NK, GW):
                slots = [(n + w + i) % NBUF for i in range(GW)]
                arrived(slots)
                left = jnp.concatenate([h[2 * w + i] for i in range(2 * GW)], axis=1)
                right = jnp.concatenate([wbuf[s, q] for s in slots for q in range(2)], axis=0)
                more = dot(left, right)
                total = more if total is None else total + more
                for i, s in enumerate(slots):
                    if c == 0:
                        fetch_down(e, 2, w + i, s)
                    else:
                        fetch_up((e + 1) % 2, 0, (c - 1) * NK + w + i, s)
            oacc[...] = total

            @pl.loop(0, N // 2)
            def _(p):
                rows = pl.ds(pl.multiple_of(p * 2 * C, 8), 2 * C)
                a, b = swap(oacc[rows, :QD], oacc[rows, QD:], first)
                rsend[e, c, 2 * p] = a.astype(jnp.bfloat16)
                rsend[e, c, 2 * p + 1] = b.astype(jnp.bfloat16)

            for i in range(N - 1):
                back(e, c, i + i // 8).start()

            rrecv[e, c, me] = rsend[e, c, me]

    @pl.loop(0, NBUF)
    def _(s):
        arrived([s])

    def sent(copies):
        @pl.loop(0, N - 1)
        def _(i):
            to = (me + 1 + i) % N
            for src, sem, e, part in copies:
                pltpu.make_async_remote_copy(
                    src.at[e, part, to], src.at[e, part, to], sem.at[e, part, to], rsem.at[e, part, to],
                    device_id=(dp, to), device_id_type=MESH,
                ).wait_send()

    sent([(send, ssem, e, part) for e in range(2) for part in range(NH)])
    sent([(rsend, rssem, 0, part) for part in range(NH)])

    for c in range(NH):
        @pl.loop(0, N - 1)
        def _(i):
            src = (me + 1 + i) % N
            for e in range(2):
                pltpu.make_async_remote_copy(
                    rsend.at[e, c, src], rrecv.at[e, c, src], rssem.at[e, c, src], rrsem.at[e, c, src],
                    device_id=(dp, src), device_id_type=MESH,
                ).wait_recv()

        @pl.loop(0, N // 2)
        def _(p):
            parts = [
                swap(rrecv[0, c, 2 * p + i].astype(jnp.float32), rrecv[1, c, 2 * p + i].astype(jnp.float32), first)
                for i in range(2)
            ]
            rows = pl.ds(pl.multiple_of(p * 4 * C, 16), 4 * C)
            for i in range(2):
                obuf[rows, i * QD : (i + 1) * QD] = jnp.concatenate(
                    [parts[0][i], parts[1][i]], axis=0
                ).astype(jnp.bfloat16)

        sent([(rsend, rssem, 1, c)])
        y_ref[:, c * KD : (c + 1) * KD] = lax.dot_general(
            ct[...], obuf[...], (((0,), (0,)), ((), ())), preferred_element_type=jnp.float32
        ).astype(jnp.bfloat16)


def solution(mesh):
    spec = P("dp", "ep")

    def layer(x, expert, slot, gate, w_gate, w_up, w_down):
        vmem = pl.BlockSpec(memory_space=pltpu.VMEM)
        hbm = pl.BlockSpec(memory_space=pl.ANY)
        bf16, f32 = jnp.bfloat16, jnp.float32
        dma = pltpu.SemaphoreType.DMA
        y = pl.pallas_call(
            kernel,
            out_shape=jax.ShapeDtypeStruct((T, D), bf16),
            in_specs=[vmem] * 4 + [hbm] * 3,
            out_specs=vmem,
            scratch_shapes=[
                pltpu.VMEM((2, NH, N, 2 * C, QD), bf16),
                pltpu.VMEM((2, NH, N, 2 * C, QD), bf16),
                pltpu.VMEM((2, NH, N, 2 * C, QD), bf16),
                pltpu.VMEM((2, NH, N, 2 * C, QD), bf16),
                pltpu.VMEM((2 * ROWS, KD), f32),
                pltpu.VMEM((ROWS, KD), bf16),
                pltpu.VMEM((NJ, 2, ROWS, TF), f32),
                pltpu.VMEM((NJ, ROWS, TF), bf16),
                pltpu.VMEM((ROWS, KD), f32),
                pltpu.VMEM((2 * ROWS, KD), bf16),
                pltpu.VMEM((2 * ROWS, T), bf16),
                pltpu.VMEM((NBUF, 2, KD, TF), bf16),
                dma((NBUF, 2)),
                dma((2, NH, N)),
                dma((2, NH, N)),
                dma((2, NH, N)),
                dma((2, NH, N)),
            ],
            compiler_params=pltpu.CompilerParams(
                collective_id=0, has_side_effects=True, vmem_limit_bytes=67_000_000
            ),
            name="moe",
        )(
            expert.reshape(T, 2).T, slot.reshape(T, 2).T, gate.reshape(T, 2).T,
            x.reshape(T, D), w_gate, w_up, w_down,
        )
        return y.reshape(1, 1, T, D)

    return jax.shard_map(
        layer, mesh=mesh,
        in_specs=(spec, spec, spec, spec, P("ep"), P("ep"), P("ep")),
        out_specs=spec, check_vma=False,
    )
```
